32 devices in a mesh: ta: 2 (over x), sa: 16 (over z, y, core).
Axes of the slice: x: 2, y: 2, z: 4, core: 2. Of those that a mesh axis runs over, the one named last changes fastest.
Arguments:
- eigvecs: bfloat16 [12, 2, 3, 6912, 128], P('ta', None, None, 'sa'), may hold values from -0.0390625 to 0.0390625
- solutions: bfloat16 [12, 2, 3, 6912, 128], P('ta', None, None, 'sa'), may hold values from -6 to 6
Outputs:
- tau: float32 [12, 2, 128, 128], P('ta', None, 'sa')
- corr: float32 [12], replicated
The draws below stay inside these ranges and needn't reach their ends.
All inputs are finite; a program needn't handle non-finite values.
Results may differ from the reference program's by a relative error of at most 0.0003.
Values sent between devices are 32-bit elements; how exact they have to be, the bound alone decides.
A program may use at most 64 MiB of HBM per device.

```python
import jax
import jax.numpy as jnp
from jax import lax

NEV = 128
NB = 128
NT = 12
SITES = 6912


def strengthened(entries, stream_key, source, target, parts, factor):
    def block_of(position):
        return (jnp.arange(entries.shape[position]) // (entries.shape[position] // parts)).reshape((-1,) + (1,) * (entries.ndim - 1 - position))

    near = jax.random.permutation(stream_key, parts)[block_of(target)]
    second = (block_of(target) + parts // 2) % parts
    return jnp.where((block_of(source) == near) | (block_of(source) == second), factor * entries, entries)


def steps_of(own_key, dims, split, smallest, top_value):
    loudness = 1.0
    for position, blocks in split:
        draws = jax.random.uniform(jax.random.fold_in(jax.random.fold_in(own_key, 6), position), (blocks,), jnp.float32, smallest / len(split), top_value / len(split))
        loudness = loudness * jnp.repeat(jnp.exp(draws), dims[position] // blocks).reshape((-1,) + (1,) * (len(dims) - 1 - position))
    return loudness


def bell_draw(stream_key, extent, deviation, reach, cuts=(), kind=jnp.bfloat16):
    drawn = deviation * jax.random.normal(stream_key, extent, jnp.float32)
    if cuts:
        drawn = drawn * steps_of(stream_key, extent, cuts, -0.22, 0.18)
    return jnp.clip(drawn, -reach, reach).astype(kind)


def gaussian_with(own_key, dims, width, bound, shards, heavy, dtype=jnp.bfloat16):
    drawn = width * jax.random.normal(own_key, dims, jnp.float32)
    if shards:
        drawn = drawn * steps_of(own_key, dims, shards, -0.22, 0.18)
    return jnp.clip(strengthened(drawn, jax.random.fold_in(own_key, 3), *heavy), -bound, bound).astype(dtype)


def setup_inputs(seed: int = 0) -> dict:
    splits = jax.random.split(jax.random.key(seed), 3)
    return {
        "eigvecs": gaussian_with(splits[0], (NT, 2, 3, SITES, NEV), (6 * SITES) ** -0.5, 0.0390625, ((0, 2), (3, 16)), (3, 4, 16, 2.0)),
        "solutions": bell_draw(splits[1], (NT, 2, 3, SITES, NB), 1.0, 6.0, ((0, 2), (3, 16))),
    }


def contract(left, right):
    return lax.dot_general(left, right, (((0,), (0,)), ((), ())), preferred_element_type=jnp.float32)


def one_slice(pair):
    vecs, sols = pair
    vec_re = vecs[0].reshape(-1, vecs.shape[-1])
    vec_im = vecs[1].reshape(-1, vecs.shape[-1])
    sol_re = sols[0].reshape(-1, sols.shape[-1])
    sol_im = sols[1].reshape(-1, sols.shape[-1])
    real_part = contract(vec_re, sol_re) + contract(vec_im, sol_im)
    imag_part = contract(vec_re, sol_im) - contract(vec_im, sol_re)
    return jnp.stack([real_part, imag_part], 0)


def reference(eigvecs, solutions):
    tau = lax.map(one_slice, (eigvecs, solutions))
    corr = jnp.sum(tau * tau, axis=(1, 2, 3)) / (2.0 * NEV * NB)
    return tau, corr
```

```python
import functools

import jax
import jax.numpy as jnp
from jax import lax
from jax.experimental import pallas as pl
from jax.experimental.pallas import tpu as pltpu
from jax.sharding import PartitionSpec as P

LANES = 128


def split_of(n):
    cores = 2 if n % 2 == 0 else 1
    rest = n // cores
    ys = 1
    while rest % (ys * 2) == 0 and (ys * 2) * (ys * 2) <= rest:
        ys *= 2
    return rest // ys, ys, cores


def kernel(dims, vec_hbm, sol_hbm, tau_ref, corr_ref,
           vec, sol, part, got_core, half, got_y, quarter, got_z, norms,
           load_sem, core_send, core_recv, y_send, y_recv, z_send, z_recv, n_send, n_recv):
    n_ta, n_sa, zs, ys, cores = dims
    slices = vec_hbm.shape[0]
    rows = tau_ref.shape[2]
    ta, me = lax.axis_index("ta"), lax.axis_index("sa")
    core = lax.rem(me, cores)
    my_y = lax.rem(me // cores, ys)
    my_z = me // (cores * ys)

    def core_peer(j):
        return me - core + lax.rem(core + j, cores)

    def y_peer(j):
        return lax.rem(my_y + j, ys)

    def z_peer(j):
        return lax.rem(my_z + j, zs)

    def at(z, y, c):
        return (z * ys + y) * cores + c

    loads = []
    for t in range(slices):
        pair = (pltpu.make_async_copy(vec_hbm.at[t], vec.at[t], load_sem.at[t, 0]),
                pltpu.make_async_copy(sol_hbm.at[t], sol.at[t], load_sem.at[t, 1]))
        for one in pair:
            one.start()
        loads.append(pair)

    barrier = pltpu.get_barrier_semaphore()
    greeted = 0
    for j in range(1, cores):
        pl.semaphore_signal(barrier, inc=1, device_id={"ta": ta, "sa": core_peer(j)})
        greeted += 1
    for j in range(1, ys):
        pl.semaphore_signal(barrier, inc=1, device_id={"ta": ta, "sa": at(my_z, y_peer(j), core)})
        greeted += 1
    for j in range(1, zs):
        pl.semaphore_signal(barrier, inc=1, device_id={"ta": ta, "sa": at(z_peer(j), my_y, core)})
        greeted += 1
    for j in range(1, n_ta):
        pl.semaphore_signal(barrier, inc=1, device_id={"ta": lax.rem(ta + j, n_ta), "sa": me})
        greeted += 1

    def core_copies(t):
        return [pltpu.make_async_remote_copy(
            src_ref=part.at[t, lax.rem(core + j, cores)], dst_ref=got_core.at[t, j - 1],
            send_sem=core_send.at[t, j - 1], recv_sem=core_recv.at[t, j - 1],
            device_id={"ta": ta, "sa": core_peer(j)}) for j in range(1, cores)]

    def y_copies(t):
        return [pltpu.make_async_remote_copy(
            src_ref=half.at[t, y_peer(j)], dst_ref=got_y.at[t, j - 1],
            send_sem=y_send.at[t, j - 1], recv_sem=y_recv.at[t, j - 1],
            device_id={"ta": ta, "sa": at(my_z, y_peer(j), core)}) for j in range(1, ys)]

    def z_copies(t):
        return [pltpu.make_async_remote_copy(
            src_ref=quarter.at[t, z_peer(j)], dst_ref=got_z.at[t, j - 1],
            send_sem=z_send.at[t, j - 1], recv_sem=z_recv.at[t, j - 1],
            device_id={"ta": ta, "sa": at(z_peer(j), my_y, core)}) for j in range(1, zs)]

    def compute(t):
        for one in loads[t]:
            one.wait()
        flat = (-1, vec.shape[-1])
        left = jnp.concatenate([vec[t, 0].reshape(flat), vec[t, 1].reshape(flat)], axis=1)
        right = jnp.concatenate([sol[t, 0].reshape(flat), sol[t, 1].reshape(flat)], axis=1)
        full = lax.dot_general(left, right, (((0,), (0,)), ((), ())), preferred_element_type=jnp.float32)
        nev, nb = vec.shape[-1], sol.shape[-1]
        both = (full[:nev, :nb] + full[nev:, nb:], full[:nev, nb:] - full[nev:, :nb])
        for p in range(2):
            for d in range(n_sa):
                c, y, z = d % cores, d // cores % ys, d // (cores * ys)
                part[t, c, y, z, p] = both[p][d * rows:(d + 1) * rows]
        if t == 0:
            pl.semaphore_wait(barrier, greeted)
        for one in core_copies(t):
            one.start()

    def after_core(t):
        for one in core_copies(t):
            one.wait_recv()
        total = part[t, core]
        for j in range(1, cores):
            total = total + got_core[t, j - 1]
        half[t] = total
        for one in y_copies(t):
            one.start()

    def after_y(t):
        for one in y_copies(t):
            one.wait_recv()
        total = half[t, my_y]
        for j in range(1, ys):
            total = total + got_y[t, j - 1]
        quarter[t] = total
        for one in z_copies(t):
            one.start()

    def after_z(t):
        for one in z_copies(t):
            one.wait_recv()
        total = quarter[t, my_z]
        for j in range(1, zs):
            total = total + got_z[t, j - 1]
        tau_ref[t] = total
        square = total * total
        return jnp.sum(square[0] + square[1], axis=0, keepdims=True)

    lag = 2
    for t in range(slices + lag):
        if t < slices:
            compute(t)
        if t >= lag:
            after_core(t - lag)
    for t in range(slices):
        after_y(t)
    width = norms.shape[-1]
    lane = lax.broadcasted_iota(jnp.int32, (1, width), 1)
    mine = jnp.zeros((1, width), jnp.float32)
    for t in range(slices):
        norm = jnp.sum(after_z(t), axis=1, keepdims=True)
        mine = mine + jnp.where(lane == ta * slices + t, norm, 0.0)
    place = ta * n_sa + me
    norms[place] = mine
    everyone = n_ta * n_sa

    def norm_copy(j):
        peer = lax.rem(place + j, everyone)
        return pltpu.make_async_remote_copy(
            src_ref=norms.at[place], dst_ref=norms.at[place],
            send_sem=n_send, recv_sem=n_recv,
            device_id={"ta": peer // n_sa, "sa": lax.rem(peer, n_sa)})

    @pl.loop(1, everyone)
    def _(j):
        norm_copy(j).start()

    for t in range(slices):
        for one in core_copies(t) + y_copies(t) + z_copies(t):
            one.wait_send()
    rest = norms.at[pl.ds(0, everyone - 1)]
    whole = pltpu.make_async_remote_copy(
        src_ref=rest, dst_ref=rest, send_sem=n_send, recv_sem=n_recv,
        device_id={"ta": ta, "sa": core_peer(1)})
    whole.wait_recv()
    scale = 1.0 / (2.0 * vec.shape[-1] * sol.shape[-1])
    corr_ref[...] = jnp.sum(norms[...], axis=0) * scale
    whole.wait_send()


def solution(mesh):
    n_ta, n_sa = mesh.shape["ta"], mesh.shape["sa"]
    zs, ys, cores = split_of(n_sa)

    def per_device(vecs, sols):
        slices, nev, nb = vecs.shape[0], vecs.shape[-1], sols.shape[-1]
        rows = nev // n_sa
        width = -(-n_ta * slices // LANES) * LANES
        f32 = jnp.float32
        block = (2, rows, nb)
        dma = pltpu.SemaphoreType.DMA
        tau, corr = pl.pallas_call(
            functools.partial(kernel, (n_ta, n_sa, zs, ys, cores)),
            out_shape=(jax.ShapeDtypeStruct((slices, 2, rows, nb), f32),
                       jax.ShapeDtypeStruct((1, width), f32)),
            in_specs=[pl.BlockSpec(memory_space=pltpu.HBM)] * 2,
            out_specs=[pl.BlockSpec(memory_space=pltpu.VMEM)] * 2,
            scratch_shapes=[
                pltpu.VMEM(vecs.shape, vecs.dtype),
                pltpu.VMEM(sols.shape, sols.dtype),
                pltpu.VMEM((slices, cores, ys, zs) + block, f32),
                pltpu.VMEM((slices, max(cores - 1, 1), ys, zs) + block, f32),
                pltpu.VMEM((slices, ys, zs) + block, f32),
                pltpu.VMEM((slices, max(ys - 1, 1), zs) + block, f32),
                pltpu.VMEM((slices, zs) + block, f32),
                pltpu.VMEM((slices, max(zs - 1, 1)) + block, f32),
                pltpu.VMEM((n_ta * n_sa, 1, width), f32),
                dma((slices, 2)),
                dma((slices, max(cores - 1, 1))), dma((slices, max(cores - 1, 1))),
                dma((slices, max(ys - 1, 1))), dma((slices, max(ys - 1, 1))),
                dma((slices, max(zs - 1, 1))), dma((slices, max(zs - 1, 1))),
                dma, dma,
            ],
            compiler_params=pltpu.CompilerParams(
                collective_id=0, has_side_effects=True, vmem_limit_bytes=48 * 1024 * 1024),
        )(vecs, sols)
        return tau, corr[0, :n_ta * slices]

    in_specs = (P("ta", None, None, "sa", None), P("ta", None, None, "sa", None))
    out_specs = (P("ta", None, "sa", None), P())
    return jax.shard_map(per_device, mesh=mesh, in_specs=in_specs, out_specs=out_specs, check_vma=False)
```

```python
import functools

import jax
import jax.numpy as jnp
from jax import lax
from jax.experimental import pallas as pl
from jax.experimental.pallas import tpu as pltpu
from jax.sharding import PartitionSpec as P

LANES = 128


def split_of(n):
    cores = 2 if n % 2 == 0 else 1
    rest = n // cores
    ys = 1
    while rest % (ys * 2) == 0 and (ys * 2) * (ys * 2) <= rest:
        ys *= 2
    return rest // ys, ys, cores


def z_first(t):
    return t % 2 == 1 and t < 4


def put_outputs(tau_in, corr_in, tau_out, corr_out, sem):
    copy = pltpu.make_async_copy(tau_in, tau_out, sem)
    copy.start()
    corr_out[...] = corr_in[0, :corr_out.shape[0]]
    copy.wait()


def kernel(dims, vec_hbm, sol_hbm, tau_ref, corr_ref,
           vec, sol, part, got_core, half, got_first, quarter, got_second, norms,
           load_sem, core_send, core_recv, first_send, first_recv, second_send, second_recv, n_send, n_recv):
    n_ta, n_sa, zs, ys, cores = dims
    slices = vec_hbm.shape[0]
    rows = tau_ref.shape[2]
    ta, me = lax.axis_index("ta"), lax.axis_index("sa")
    core = lax.rem(me, cores)
    my_y = lax.rem(me // cores, ys)
    my_z = me // (cores * ys)

    def core_peer(j):
        return me - core + lax.rem(core + j, cores)

    def y_peer(j):
        return lax.rem(my_y + j, ys)

    def z_peer(j):
        return lax.rem(my_z + j, zs)

    def at(z, y, c):
        return (z * ys + y) * cores + c

    loads = []
    for t in range(slices):
        pair = (pltpu.make_async_copy(vec_hbm.at[t], vec.at[t], load_sem.at[t, 0]),
                pltpu.make_async_copy(sol_hbm.at[t], sol.at[t], load_sem.at[t, 1]))
        for one in pair:
            one.start()
        loads.append(pair)

    barrier = pltpu.get_barrier_semaphore()
    greeted = 0
    for j in range(1, cores):
        pl.semaphore_signal(barrier, inc=1, device_id={"ta": ta, "sa": core_peer(j)})
        greeted += 1
    for j in range(1, ys):
        pl.semaphore_signal(barrier, inc=1, device_id={"ta": ta, "sa": at(my_z, y_peer(j), core)})
        greeted += 1
    for j in range(1, zs):
        pl.semaphore_signal(barrier, inc=1, device_id={"ta": ta, "sa": at(z_peer(j), my_y, core)})
        greeted += 1
    for j in range(1, n_ta):
        pl.semaphore_signal(barrier, inc=1, device_id={"ta": lax.rem(ta + j, n_ta), "sa": me})
        greeted += 1

    def core_copies(t):
        return [pltpu.make_async_remote_copy(
            src_ref=part.at[t, lax.rem(core + j, cores)], dst_ref=got_core.at[t, j - 1],
            send_sem=core_send.at[t, j - 1], recv_sem=core_recv.at[t, j - 1],
            device_id={"ta": ta, "sa": core_peer(j)}) for j in range(1, cores)]

    def axes_of(t):
        y_axis, z_axis = (my_y, ys, y_peer), (my_z, zs, z_peer)
        return (z_axis, y_axis) if z_first(t) else (y_axis, z_axis)

    def device_of(t, stage, position):
        along_z = z_first(t) == (stage == 0)
        return {"ta": ta, "sa": at(position, my_y, core) if along_z else at(my_z, position, core)}

    def first_copies(t):
        (_, size, peer), (_, other, _) = axes_of(t)
        return [pltpu.make_async_remote_copy(
            src_ref=half.at[t, pl.ds(peer(j) * other, other)], dst_ref=got_first.at[t, pl.ds((j - 1) * other, other)],
            send_sem=first_send.at[t, j - 1], recv_sem=first_recv.at[t, j - 1],
            device_id=device_of(t, 0, peer(j))) for j in range(1, size)]

    def second_copies(t):
        _, (_, size, peer) = axes_of(t)
        return [pltpu.make_async_remote_copy(
            src_ref=quarter.at[t, peer(j)], dst_ref=got_second.at[t, j - 1],
            send_sem=second_send.at[t, j - 1], recv_sem=second_recv.at[t, j - 1],
            device_id=device_of(t, 1, peer(j))) for j in range(1, size)]

    def compute(t):
        for one in loads[t]:
            one.wait()
        flat = (-1, vec.shape[-1])
        left = jnp.concatenate([vec[t, 0].reshape(flat), vec[t, 1].reshape(flat)], axis=1)
        right = jnp.concatenate([sol[t, 0].reshape(flat), sol[t, 1].reshape(flat)], axis=1)
        full = lax.dot_general(left, right, (((0,), (0,)), ((), ())), preferred_element_type=jnp.float32)
        nev, nb = vec.shape[-1], sol.shape[-1]
        both = (full[:nev, :nb] + full[nev:, nb:], full[:nev, nb:] - full[nev:, :nb])
        for p in range(2):
            for d in range(n_sa):
                c, y, z = d % cores, d // cores % ys, d // (cores * ys)
                part[t, c, z * ys + y if z_first(t) else y * zs + z, p] = both[p][d * rows:(d + 1) * rows]
        if t == 0:
            pl.semaphore_wait(barrier, greeted)
        for one in core_copies(t):
            one.start()

    def after_core(t):
        for one in core_copies(t):
            one.wait_recv()
        total = part[t, core]
        for j in range(1, cores):
            total = total + got_core[t, j - 1]
        half[t] = total
        for one in first_copies(t):
            one.start()

    def after_first(t):
        for one in first_copies(t):
            one.wait_recv()
        (own, size, _), (_, other, _) = axes_of(t)
        total = half[t, pl.ds(own * other, other)]
        for j in range(1, size):
            total = total + got_first[t, (j - 1) * other:j * other]
        quarter[t, :other] = total
        for one in second_copies(t):
            one.start()

    def after_second(t):
        for one in second_copies(t):
            one.wait_recv()
        _, (own, size, _) = axes_of(t)
        total = quarter[t, own]
        for j in range(1, size):
            total = total + got_second[t, j - 1]
        tau_ref[t] = total
        square = total * total
        return jnp.sum(square[0] + square[1], axis=0, keepdims=True)

    lag = 2
    for t in range(slices + lag):
        if t < slices:
            compute(t)
        if t >= lag:
            after_core(t - lag)
    for t in range(slices):
        after_first(t)
    width = norms.shape[-1]
    lane = lax.broadcasted_iota(jnp.int32, (1, width), 1)
    mine = jnp.zeros((1, width), jnp.float32)
    for t in range(slices):
        norm = jnp.sum(after_second(t), axis=1, keepdims=True)
        mine = mine + jnp.where(lane == ta * slices + t, norm, 0.0)
    place = ta * n_sa + me
    norms[place] = mine
    everyone = n_ta * n_sa

    def norm_copy(j):
        peer = lax.rem(place + j, everyone)
        return pltpu.make_async_remote_copy(
            src_ref=norms.at[place], dst_ref=norms.at[place],
            send_sem=n_send, recv_sem=n_recv,
            device_id={"ta": peer // n_sa, "sa": lax.rem(peer, n_sa)})

    @pl.loop(1, everyone)
    def _(j):
        norm_copy(j).start()

    for t in range(slices):
        for one in core_copies(t) + first_copies(t) + second_copies(t):
            one.wait_send()
    rest = norms.at[pl.ds(0, everyone - 1)]
    whole = pltpu.make_async_remote_copy(
        src_ref=rest, dst_ref=rest, send_sem=n_send, recv_sem=n_recv,
        device_id={"ta": ta, "sa": core_peer(1)})
    whole.wait_recv()
    scale = 1.0 / (2.0 * vec.shape[-1] * sol.shape[-1])
    corr_ref[...] = jnp.sum(norms[...], axis=0) * scale
    whole.wait_send()


def solution(mesh):
    n_ta, n_sa = mesh.shape["ta"], mesh.shape["sa"]
    zs, ys, cores = split_of(n_sa)

    def per_device(vecs, sols):
        slices, nev, nb = vecs.shape[0], vecs.shape[-1], sols.shape[-1]
        rows = nev // n_sa
        width = -(-n_ta * slices // LANES) * LANES
        f32 = jnp.float32
        block = (2, rows, nb)
        dma = pltpu.SemaphoreType.DMA
        tau, corr = pl.pallas_call(
            functools.partial(kernel, (n_ta, n_sa, zs, ys, cores)),
            out_shape=(jax.ShapeDtypeStruct((slices, 2, rows, nb), f32),
                       jax.ShapeDtypeStruct((1, width), f32)),
            in_specs=[pl.BlockSpec(memory_space=pltpu.HBM)] * 2,
            out_specs=[pl.BlockSpec(memory_space=pltpu.VMEM)] * 2,
            scratch_shapes=[
                pltpu.VMEM(vecs.shape, vecs.dtype),
                pltpu.VMEM(sols.shape, sols.dtype),
                pltpu.VMEM((slices, cores, ys * zs) + block, f32),
                pltpu.VMEM((slices, max(cores - 1, 1), ys * zs) + block, f32),
                pltpu.VMEM((slices, ys * zs) + block, f32),
                pltpu.VMEM((slices, ys * zs) + block, f32),
                pltpu.VMEM((slices, max(ys, zs)) + block, f32),
                pltpu.VMEM((slices, max(ys, zs)) + block, f32),
                pltpu.VMEM((n_ta * n_sa, 1, width), f32),
                dma((slices, 2)),
                dma((slices, max(cores - 1, 1))), dma((slices, max(cores - 1, 1))),
                dma((slices, max(ys, zs))), dma((slices, max(ys, zs))),
                dma((slices, max(ys, zs))), dma((slices, max(ys, zs))),
                dma, dma,
            ],
            compiler_params=pltpu.CompilerParams(
                collective_id=0, has_side_effects=True, vmem_limit_bytes=64_000_000),
        )(vecs, sols)
        return pl.pallas_call(
            put_outputs,
            out_shape=(jax.ShapeDtypeStruct(tau.shape, f32), jax.ShapeDtypeStruct((n_ta * slices,), f32)),
            in_specs=[pl.BlockSpec(memory_space=pltpu.VMEM)] * 2,
            out_specs=[pl.BlockSpec(memory_space=pltpu.HBM), pl.BlockSpec(memory_space=pltpu.VMEM)],
            scratch_shapes=[dma],
        )(tau, corr)

    in_specs = (P("ta", None, None, "sa", None), P("ta", None, None, "sa", None))
    out_specs = (P("ta", None, "sa", None), P())
    return jax.shard_map(per_device, mesh=mesh, in_specs=in_specs, out_specs=out_specs, check_vma=False)
```
